32 devices in a mesh: grp: 4 (over z), col: 8 (over y, x, core).
Axes of the slice: x: 2, y: 2, z: 4, core: 2. Of those that a mesh axis runs over, the one named last changes fastest.
Arguments:
- x_blocks: bfloat16 [16, 8, 6, 256, 256], P('grp', 'col'), may hold values from -6 to 6
- columns: int32 [16, 8, 6], replicated, may hold values from -1 to 127, as said below
- filter_ids: int32 [16, 8, 6], replicated, may hold values from 0 to 127, as said below
Outputs:
- sign_step: bfloat16 [16, 8, 6, 256, 256], P('grp', 'col')
The draws below stay inside these ranges and needn't reach their ends.
Inputs may be any that keep to these rules, and one draw needn't show every extreme that they name: `columns`: in each block row of the grid, slot 0 holds the row's own id; the other used slots hold distinct ids of block rows at most one step away along each grid dimension, with periodic wrap; used slots come first, then -1; at least 3 slots are used. `filter_ids`: in each block row, slot 0 holds the row's own id and the others distinct ids of block rows at most one step away along each grid dimension, with periodic wrap.
All inputs are finite; a program needn't handle non-finite values.
Results may differ from the reference program's by a relative error of at most 0.0019.
Values may be sent and summed in bfloat16 or wider, within the bound.
A program may use at most 128 MiB of HBM per device.

```python
import jax
import jax.numpy as jnp
from jax import lax

B = 256
KB = 6
KF = 6
NA = 16
NBC = 8


def neighbour_ids(key, slots):
    total_rows = NA * NBC
    row_keys = jax.random.split(key, total_rows)
    shuffled = jax.vmap(lambda one_key: jax.random.permutation(one_key, 8))(row_keys)
    others = shuffled + (shuffled >= 4).astype(shuffled.dtype)
    offset_code = jnp.concatenate([jnp.full((total_rows, 1), 4, jnp.int32), others.astype(jnp.int32)], axis=1)[:, :slots]
    step_a = offset_code // 3 - 1
    step_c = offset_code % 3 - 1
    row_index = jnp.arange(total_rows, dtype=jnp.int32)
    home_a = row_index // NBC
    home_c = row_index % NBC
    block_ids = (home_a[:, None] + step_a) % NA * NBC + (home_c[:, None] + step_c) % NBC
    return block_ids.astype(jnp.int32)


def draw_columns(key, part):
    total_rows = NA * NBC
    block_ids = neighbour_ids(jax.random.fold_in(key, 11), KB)
    counts = jax.random.randint(jax.random.fold_in(key, 12), (total_rows, 1), 3, KB + 1)
    slot_index = jnp.arange(KB, dtype=jnp.int32)[None, :]
    block_ids = jnp.where(slot_index < counts, block_ids, -1)
    return block_ids.reshape(NA, NBC, KB).astype(jnp.int32)


def draw_filter_ids(key, part):
    block_ids = neighbour_ids(jax.random.fold_in(key, 21), KF)
    return block_ids.reshape(NA, NBC, KF).astype(jnp.int32)


def level_of(stream_key, shape, pieces, low, top_value):
    gain = 1.0
    for axis_at, blocks in pieces:
        draws = jax.random.uniform(jax.random.fold_in(jax.random.fold_in(stream_key, 6), axis_at), (blocks,), jnp.float32, low / len(pieces), top_value / len(pieces))
        gain = gain * jnp.repeat(jnp.exp(draws), shape[axis_at] // blocks).reshape((-1,) + (1,) * (len(shape) - 1 - axis_at))
    return gain


def bell_draw(key, shape, scale, most, cuts=(), kind=jnp.bfloat16):
    loudness = level_of(key, shape, cuts, -0.22, 0.18) if cuts else 1.0
    values = jax.random.normal(key, shape, jnp.float32) * scale * loudness
    return jnp.minimum(jnp.maximum(values, -most), most).astype(kind)


def setup_inputs(seed: int = 0) -> dict:
    key_of = jax.random.split(jax.random.key(seed), 4)
    return {
        "x_blocks": bell_draw(key_of[0], (NA, NBC, KB, B, B), 1.0, 6.0, ((0, 4), (1, 8))),
        "columns": draw_columns(jax.random.fold_in(key_of[3], 71), 0),
        "filter_ids": draw_filter_ids(jax.random.fold_in(key_of[3], 71), 0),
    }


def locate(stored, wanted):
    matches = stored[:, None, :] == wanted[None, :, None]
    present = jnp.any(matches, axis=2) & (wanted[None, :] >= 0)
    slot_of = jnp.argmax(matches.astype(jnp.int32), axis=2).astype(jnp.int32)
    return slot_of, present


def reference(x_blocks, columns, filter_ids):
    total_rows = NA * NBC
    blocks = x_blocks.reshape(total_rows, KB, B, B)
    col_table = columns.reshape(total_rows, KB)
    filt_table = filter_ids.reshape(total_rows, KF)

    def square_row(row_index):
        row_cols = col_table[row_index]
        in_use = row_cols >= 0
        source = jnp.where(in_use, row_cols, 0)
        slot_of, present = locate(col_table[source], filt_table[row_index])
        present = present & in_use[:, None]
        picked = blocks[source[:, None], slot_of].astype(jnp.float32) * present[:, :, None, None].astype(jnp.float32)
        own = blocks[row_index].astype(jnp.float32)
        return jnp.einsum("kab,kfbc->fac", own, picked).astype(jnp.bfloat16)

    square = lax.map(square_row, jnp.arange(total_rows, dtype=jnp.int32))

    def sign_row(row_index):
        row_cols = col_table[row_index]
        in_use = row_cols >= 0
        source = jnp.where(in_use, row_cols, 0)
        slot_of, present = locate(filt_table[source], row_cols)
        present = present & in_use[:, None]
        picked = square[source[:, None], slot_of].astype(jnp.float32) * present[:, :, None, None].astype(jnp.float32)
        own = blocks[row_index].astype(jnp.float32)
        cubed = jnp.einsum("kab,kjbc->jac", own, picked)
        result = (1.5 * own - cubed * (0.5 / (KB * B))) * in_use[:, None, None].astype(jnp.float32)
        return result.astype(jnp.bfloat16)

    updated = lax.map(sign_row, jnp.arange(total_rows, dtype=jnp.int32))
    return updated.reshape(NA, NBC, KB, B, B)
```

```python
import functools

import jax
import jax.numpy as jnp
from jax import lax
from jax.experimental import pallas as pl
from jax.experimental.pallas import tpu as pltpu
from jax.sharding import PartitionSpec as P

MESH = pl.DeviceIdType.MESH
STEPS = [(da, dc) for da in (-1, 0, 1) for dc in (-1, 0, 1)]
FLOWS = [(0, -1), (0, 1), (-1, 0), (1, 0), (-1, -1), (-1, 1), (1, -1), (1, 1)]
LIMIT = 48 * 1024 * 1024


def flow_bases(rows, slots):
    sizes = [rows * slots] * 2 + [slots] * 6
    bases = [sum(sizes[:i]) for i in range(8)]
    return bases, sum(sizes)


def grid_maps(shape, grid_a, grid_c, rows):
    rid = lax.broadcasted_iota(jnp.int32, shape, 1)
    a = jnp.zeros_like(rid)
    for i in range(1, grid_a):
        a = a + (rid >= i * grid_c).astype(jnp.int32)
    group = jnp.zeros_like(rid)
    for i in range(1, grid_a // rows):
        group = group + (a >= i * rows).astype(jnp.int32)
    return rid, rid - a * grid_c, a - group * rows


def shifted(x, step, col, grid_c, roll):
    da, dc = step
    if da:
        x = roll(x, -da * grid_c, 1)
    if dc == 1:
        x = jnp.where(col == grid_c - 1, roll(x, grid_c - 1, 1), roll(x, -1, 1))
    if dc == -1:
        x = jnp.where(col == 0, roll(x, 1 - grid_c, 1), roll(x, 1, 1))
    return x


def row_of(x, i):
    return jnp.broadcast_to(x[i : i + 1], x.shape)


def chosen(cols, maps, grid_c, roll):
    rid, col, _ = maps
    hits, uses = [], []
    for step in STEPS:
        hit = (cols == shifted(rid, step, col, grid_c, roll)).astype(jnp.int32)
        hits.append(hit)
        uses.append(jnp.broadcast_to(jnp.max(hit, axis=0, keepdims=True), cols.shape))
    return hits, uses


def tables(stored, wanted, hits, uses, maps, rows, grid_c, slots, roll):
    _, col, al = maps
    sub = lax.broadcasted_iota(jnp.int32, stored.shape, 0)
    bases, _ = flow_bases(rows, slots)
    sh = functools.partial(shifted, col=col, grid_c=grid_c, roll=roll)
    need = {flow: jnp.zeros_like(stored) for flow in FLOWS}
    side = {}
    for i, (da, dc) in enumerate(STEPS):
        back = (-da, -dc)
        asked = sh(wanted, back)
        hit = jnp.zeros_like(stored)
        for f in range(slots):
            hit = hit | (stored == row_of(asked, f)).astype(jnp.int32)
        hit = hit & sh(uses[i], back)
        for gd in (-1, 0, 1):
            if (gd, -dc) == (0, 0) or gd * da > 0 or (gd != 0 and da == 0):
                continue
            at = al - da
            inside = (at < 0) if gd < 0 else (at >= rows) if gd > 0 else (at >= 0) & (at < rows)
            side[da, dc, gd] = inside
            need[gd, -dc] = need[gd, -dc] | (hit & inside.astype(jnp.int32))
    ranks, counts = [], []
    for flow in FLOWS:
        n = need[flow]
        ahead = jnp.zeros_like(n)
        for s in range(1, slots):
            ahead = ahead + jnp.where(sub >= s, roll(n, s, 0), 0)
        total = jnp.broadcast_to(jnp.sum(n, axis=0, keepdims=True), n.shape)
        before = jnp.zeros_like(n)
        for s in range(1, rows):
            before = before + jnp.where(al >= s, roll(total, s * grid_c, 1), 0)
        ranks.append(jnp.where(n > 0, before + ahead, -1))
        counts.append(jnp.where(al == rows - 1, before + total, 0))
    own = al * slots + sub
    found = []
    for da, dc in STEPS:
        place = own if dc == 0 else jnp.full_like(own, -1)
        for gd in (-1, 0, 1):
            if (da, dc, gd) not in side:
                continue
            d = FLOWS.index((gd, -dc))
            there = jnp.where(ranks[d] >= 0, rows * slots + bases[d] + ranks[d], -1)
            place = jnp.where(side[da, dc, gd], there, place)
        place = sh(place, (da, dc))
        kept = sh(stored, (da, dc))
        loc = jnp.full_like(own, -1)
        for m in range(slots):
            loc = jnp.where(wanted == row_of(kept, m), row_of(place, m), loc)
        found.append(loc)
    locs = []
    for k in range(slots):
        loc = jnp.full_like(own, -1)
        for i in range(len(STEPS)):
            loc = jnp.where(row_of(hits[i], k) > 0, found[i], loc)
        locs.append(loc)
    return locs, ranks, counts


def level_of(counts, levels):
    sizes = []
    for group in (counts[:2], counts[2:4], counts[4:]):
        most = group[0]
        for c in group[1:]:
            most = jnp.maximum(most, c)
        sizes.append(jnp.max(most))
    out = jnp.int32(0)
    stride = 1
    for size, steps in zip(sizes, levels):
        for s in steps[:-1]:
            out = out + stride * (size > s).astype(jnp.int32)
        stride *= len(steps)
    return out


def my_lanes(rows, grid_c):
    start = lax.axis_index("grp") * rows * grid_c + lax.axis_index("col")
    return [start + i * grid_c for i in range(rows)]


def put_blocks(rank_ref, blocks, send, sem, row, lane, flows, slots, bases, total):
    for d in flows:
        for m in range(slots):
            rank = rank_ref[d * 8 + m, lane]

            @pl.when(rank >= 0)
            def _(d=d, m=m, rank=rank):
                pltpu.make_async_copy(blocks.at[row * slots + m], send.at[bases[d] + rank], sem).start()

            total = total + (rank >= 0).astype(jnp.int32)
    return total


def put_row(rank_ref, blocks, send, sem, row, lanes, rows, slots, bases, total):
    flows = [0, 1]
    if row == 0:
        flows += [2, 4, 5]
    if row == rows - 1:
        flows += [3, 6, 7]
    return put_blocks(rank_ref, blocks, send, sem, row, lanes[row], flows, slots, bases, total)


def drain(n, src, dst, sem):
    def one(_, carry):
        pltpu.make_async_copy(src, dst, sem).wait()
        return carry

    lax.fori_loop(0, n, one, 0)


def plan_kernel(
    dims, cols_ref, filt_ref, x_ref, loc1, loc2, rank2, cnt1, cnt2, level, send, rank1_v, rank1, tsem, sem
):
    rows, grid_a, grid_c, slots, levels = dims
    bases, _ = flow_bases(rows, slots)
    cols, filt = cols_ref[...], filt_ref[...]

    def roll(x, s, axis):
        return pltpu.roll(x, s % x.shape[axis], axis)

    maps = grid_maps(cols.shape, grid_a, grid_c, rows)
    hits, uses = chosen(cols, maps, grid_c, roll)
    asked = jnp.where(filt < 0, -2, filt)
    locs, ranks, counts = tables(cols, asked, hits, uses, maps, rows, grid_c, slots, roll)
    for d in range(8):
        rank1_v[d * 8 : d * 8 + 8, :] = ranks[d]
        cnt1[d : d + 1, :] = counts[d][:1]
    table = pltpu.make_async_copy(rank1_v, rank1, tsem)
    table.start()
    for k in range(slots):
        loc1[k * 8 : k * 8 + 8, :] = locs[k]
    level[0] = level_of(counts, levels)
    table.wait()
    lanes = my_lanes(rows, grid_c)
    total = jnp.int32(0)
    for row in range(rows):
        total = put_row(rank1, x_ref, send, sem, row, lanes, rows, slots, bases, total)
    asked = jnp.where(cols < 0, -2, cols)
    locs, ranks, counts = tables(filt, asked, hits, uses, maps, rows, grid_c, slots, roll)
    for d in range(8):
        rank2[d * 8 : d * 8 + 8, :] = ranks[d]
        cnt2[d : d + 1, :] = counts[d][:1]
    for k in range(slots):
        loc2[k * 8 : k * 8 + 8, :] = locs[k]
    level[1] = level_of(counts, levels)
    drain(total, x_ref.at[0], send.at[0], sem)


def swap_kernel(sizes, bases, send, recv, send_sem, recv_sem):
    grp, col = lax.axis_index("grp"), lax.axis_index("col")
    grps, cols = lax.axis_size("grp"), lax.axis_size("col")
    barrier = pltpu.get_barrier_semaphore()
    peers = [(lax.rem(grp + gd + grps, grps), lax.rem(col + dc + cols, cols)) for gd, dc in FLOWS]
    for peer in peers:
        pl.semaphore_signal(barrier, inc=1, device_id=peer, device_id_type=MESH)
    pl.semaphore_wait(barrier, 8)
    copies = []
    for d, n in enumerate(sizes):
        copy = pltpu.make_async_remote_copy(
            src_ref=send.at[pl.ds(bases[d], n)],
            dst_ref=recv.at[pl.ds(bases[d], n)],
            send_sem=send_sem.at[d],
            recv_sem=recv_sem.at[d],
            device_id=peers[d],
            device_id_type=MESH,
        )
        copy.start()
        copies.append(copy)
    for copy in copies:
        copy.wait()


def swap(send, level, levels, rows, slots, first_id):
    bases, _ = flow_bases(rows, slots)
    branches = []
    for c in levels[2]:
        for v in levels[1]:
            for l in levels[0]:
                sizes = [l] * 2 + [v] * 2 + [c] * 4
                branches.append(
                    pl.pallas_call(
                        functools.partial(swap_kernel, sizes, bases),
                        out_shape=jax.ShapeDtypeStruct(send.shape, send.dtype),
                        in_specs=[pl.BlockSpec(memory_space=pl.ANY)],
                        out_specs=pl.BlockSpec(memory_space=pl.ANY),
                        scratch_shapes=[pltpu.SemaphoreType.DMA((8,)), pltpu.SemaphoreType.DMA((8,))],
                        compiler_params=pltpu.CompilerParams(
                            collective_id=first_id + len(branches), has_side_effects=True
                        ),
                        name=f"swap_{l}_{v}_{c}",
                    )
                )
    return lax.switch(level, branches, send)


def fetch(cnt, recv, buf, sem, rows, grid_c, slots):
    bases, _ = flow_bases(rows, slots)
    grp, col = lax.axis_index("grp"), lax.axis_index("col")
    grps = lax.axis_size("grp")
    total = jnp.int32(0)
    for d, (gd, dc) in enumerate(FLOWS):
        g = lax.rem(grp - gd + grps, grps)
        c = lax.rem(col - dc + grid_c, grid_c)
        n = cnt[d, (g * rows + rows - 1) * grid_c + c]

        def one(i, carry, d=d):
            pltpu.make_async_copy(recv.at[bases[d] + i], buf.at[rows * slots + bases[d] + i], sem).start()
            return carry

        lax.fori_loop(0, n, one, 0)
        total = total + n
    return total


def products(loc, left, buf, acc, row, lane, f, slots):
    acc[...] = jnp.zeros_like(acc)
    for k in range(slots):
        at = loc[k * 8 + f, lane]

        @pl.when(at >= 0)
        def _(k=k, at=at):
            acc[...] += jnp.dot(left[row * slots + k], buf[at], preferred_element_type=jnp.float32)


def square_kernel(dims, loc, cnt, rank2, x, recv, out, send, buf, acc, xsem, sem, ssem):
    rows, grid_c, slots = dims
    bases, _ = flow_bases(rows, slots)
    mine = pltpu.make_async_copy(x, buf.at[pl.ds(0, rows * slots)], xsem)
    mine.start()
    total = fetch(cnt, recv, buf, sem, rows, grid_c, slots)
    mine.wait()
    drain(total, recv.at[0], buf.at[rows * slots], sem)
    lanes = my_lanes(rows, grid_c)
    sent = jnp.int32(0)
    for row in range(rows):

        def one(f, carry, row=row):
            products(loc, buf, buf, acc, row, lanes[row], f, slots)
            out[row * slots + f] = acc[...].astype(out.dtype)
            return carry

        lax.fori_loop(0, slots, one, 0)
        sent = put_row(rank2, out, send, ssem, row, lanes, rows, slots, bases, sent)
    drain(sent, out.at[0], send.at[0], ssem)


def cube_kernel(dims, scale, loc, cnt, cols, x, square, recv, out, buf, acc, xsem, sem):
    rows, grid_c, slots = dims
    mine = pltpu.make_async_copy(square, buf.at[pl.ds(0, rows * slots)], xsem)
    mine.start()
    total = fetch(cnt, recv, buf, sem, rows, grid_c, slots)
    mine.wait()
    drain(total, recv.at[0], buf.at[rows * slots], sem)
    lanes = my_lanes(rows, grid_c)
    for row in range(rows):

        def one(f, carry, row=row):
            products(loc, x, buf, acc, row, lanes[row], f, slots)
            used = (cols[f, lanes[row]] >= 0).astype(jnp.float32)
            value = 1.5 * x[row * slots + f].astype(jnp.float32) - acc[...] * scale
            out[row * slots + f] = (value * used).astype(out.dtype)
            return carry

        lax.fori_loop(0, slots, one, 0)


def local(x_blocks, columns, filter_ids):
    grps, ncol = lax.axis_size("grp"), lax.axis_size("col")
    rows, per_col, slots, order = x_blocks.shape[:4]
    assert per_col == 1 and filter_ids.shape[2] == slots
    grid_a, grid_c = rows * grps, per_col * ncol
    count = grid_a * grid_c
    blocks = x_blocks.reshape(rows * slots, order, order)
    _, extra = flow_bases(rows, slots)
    dtype = blocks.dtype
    wide = sorted({min(n, rows * slots) for n in (11, 12, 13, 14, 15, 16, 17, rows * slots)})
    levels = (wide, (4, 5, slots), (3, 4))

    def laid(table):
        return jnp.pad(table.reshape(count, slots).T, ((0, 8 - slots), (0, 0)), constant_values=-1)

    cols, filt = laid(columns), laid(filter_ids)
    vmem = pl.BlockSpec(memory_space=pltpu.VMEM)
    smem = pl.BlockSpec(memory_space=pltpu.SMEM)
    anyw = pl.BlockSpec(memory_space=pl.ANY)
    ints = lambda n: jax.ShapeDtypeStruct((n, count), jnp.int32)
    packed = jax.ShapeDtypeStruct((extra, order, order), dtype)
    held = jax.ShapeDtypeStruct(blocks.shape, dtype)
    dma = pltpu.SemaphoreType.DMA
    params = pltpu.CompilerParams(vmem_limit_bytes=LIMIT)

    loc1, loc2, rank2, cnt1, cnt2, level, send = pl.pallas_call(
        functools.partial(plan_kernel, (rows, grid_a, grid_c, slots, levels)),
        out_shape=[
            ints(slots * 8),
            ints(slots * 8),
            ints(64),
            ints(8),
            ints(8),
            jax.ShapeDtypeStruct((2,), jnp.int32),
            packed,
        ],
        in_specs=[vmem, vmem, vmem],
        out_specs=[vmem] * 5 + [smem, anyw],
        scratch_shapes=[pltpu.VMEM((64, count), jnp.int32), pltpu.SMEM((64, count), jnp.int32), dma(()), dma(())],
        compiler_params=params,
        name="plan",
    )(cols, filt, blocks)
    recv = swap(send, level[0], levels, rows, slots, 0)
    square, send = pl.pallas_call(
        functools.partial(square_kernel, (rows, grid_c, slots)),
        out_shape=[held, packed],
        in_specs=[smem, smem, smem, anyw, anyw],
        out_specs=[vmem, anyw],
        scratch_shapes=[
            pltpu.VMEM((rows * slots + extra, order, order), dtype),
            pltpu.VMEM((order, order), jnp.float32),
            dma(()),
            dma(()),
            dma(()),
        ],
        compiler_params=params,
        name="square",
    )(loc1, cnt1, rank2, blocks, recv)
    branches = len(levels[0]) * len(levels[1]) * len(levels[2])
    recv = swap(send, level[1], levels, rows, slots, branches)
    out = pl.pallas_call(
        functools.partial(cube_kernel, (rows, grid_c, slots), 0.5 / (slots * order)),
        out_shape=held,
        in_specs=[smem, smem, smem, vmem, anyw, anyw],
        out_specs=vmem,
        scratch_shapes=[
            pltpu.VMEM((rows * slots + extra, order, order), dtype),
            pltpu.VMEM((order, order), jnp.float32),
            dma(()),
            dma(()),
        ],
        compiler_params=params,
        name="cube",
    )(loc2, cnt2, cols, blocks, square, recv)
    return out.reshape(x_blocks.shape)


def solution(mesh):
    return jax.shard_map(
        local,
        mesh=mesh,
        in_specs=(P("grp", "col", None, None, None), P(), P()),
        out_specs=P("grp", "col", None, None, None),
        check_vma=False,
    )
```

```python
import functools

import jax
import jax.numpy as jnp
from jax import lax
from jax.experimental import pallas as pl
from jax.experimental.pallas import tpu as pltpu
from jax.sharding import PartitionSpec as P

MESH = pl.DeviceIdType.MESH
STEPS = [(da, dc) for da in (-1, 0, 1) for dc in (-1, 0, 1)]
FLOWS = [(0, -1), (0, 1), (-1, 0), (1, 0)]
PASSED = 8
STAIRS = (
    ((11, 6, 5), (12, 6, 5), (13, 6, 5), (14, 6, 6), (15, 6, 7)),
    ((14, 6, 6), (15, 6, 6), (16, 6, 6), (16, 6, 7), (18, 6, 7)),
)
LIMIT = 48 * 1024 * 1024


def flow_bases(rows, slots):
    sizes = [rows * slots] * 2 + [slots] * 2 + [PASSED] * 2
    bases = [sum(sizes[:i]) for i in range(6)]
    return bases, sum(sizes)


def grid_maps(shape, grid_a, grid_c, rows):
    rid = lax.broadcasted_iota(jnp.int32, shape, 1)
    a = jnp.zeros_like(rid)
    for i in range(1, grid_a):
        a = a + (rid >= i * grid_c).astype(jnp.int32)
    group = jnp.zeros_like(rid)
    for i in range(1, grid_a // rows):
        group = group + (a >= i * rows).astype(jnp.int32)
    return rid, rid - a * grid_c, a - group * rows


def shifted(x, step, col, grid_c, roll):
    da, dc = step
    if da:
        x = roll(x, -da * grid_c, 1)
    if dc == 1:
        x = jnp.where(col == grid_c - 1, roll(x, grid_c - 1, 1), roll(x, -1, 1))
    if dc == -1:
        x = jnp.where(col == 0, roll(x, 1 - grid_c, 1), roll(x, 1, 1))
    return x


def row_of(x, i):
    return jnp.broadcast_to(x[i : i + 1], x.shape)


def chosen(cols, maps, grid_c, roll):
    rid, col, _ = maps
    hits, uses = [], []
    for step in STEPS:
        hit = (cols == shifted(rid, step, col, grid_c, roll)).astype(jnp.int32)
        hits.append(hit)
        uses.append(jnp.broadcast_to(jnp.max(hit, axis=0, keepdims=True), cols.shape))
    return hits, uses


def tables(stored, wanted, hits, uses, maps, rows, grid_c, slots, roll):
    _, col, al = maps
    sub = lax.broadcasted_iota(jnp.int32, stored.shape, 0)
    bases, _ = flow_bases(rows, slots)
    sh = functools.partial(shifted, col=col, grid_c=grid_c, roll=roll)
    need = {(gd, dc): jnp.zeros_like(stored) for gd in (-1, 0, 1) for dc in (-1, 0, 1)}
    side = {}
    for i, (da, dc) in enumerate(STEPS):
        back = (-da, -dc)
        asked = sh(wanted, back)
        hit = jnp.zeros_like(stored)
        for f in range(slots):
            hit = hit | (stored == row_of(asked, f)).astype(jnp.int32)
        hit = hit & sh(uses[i], back)
        for gd in (-1, 0, 1):
            if (gd, -dc) == (0, 0) or gd * da > 0 or (gd != 0 and da == 0):
                continue
            at = al - da
            inside = (at < 0) if gd < 0 else (at >= rows) if gd > 0 else (at >= 0) & (at < rows)
            side[da, dc, gd] = inside
            need[gd, -dc] = need[gd, -dc] | (hit & inside.astype(jnp.int32))
    def ahead_of(n):
        ahead = jnp.zeros_like(n)
        for s in range(1, slots):
            ahead = ahead + jnp.where(sub >= s, roll(n, s, 0), 0)
        return ahead, jnp.broadcast_to(jnp.sum(n, axis=0, keepdims=True), n.shape)

    ranks, counts = [], []
    for gd, dc in FLOWS:
        n = need[gd, dc]
        if gd:
            n = n | need[gd, -1] | need[gd, 1]
        ahead, total = ahead_of(n)
        before = jnp.zeros_like(n)
        for s in range(1, rows):
            before = before + jnp.where(al >= s, roll(total, s * grid_c, 1), 0)
        ranks.append(jnp.where(n > 0, before + ahead, -1))
        counts.append(jnp.where(al == rows - 1, before + total, 0))
    passed, picks = {}, []
    for dc in (-1, 1):
        low, high = need[1, dc], need[-1, dc]
        ahead, total = ahead_of(low)
        passed[1, dc] = jnp.where(low > 0, ahead, -1)
        skip = roll(total, (rows + 1) * grid_c, 1)
        ahead, total = ahead_of(high)
        passed[-1, dc] = jnp.where(high > 0, ahead + skip, -1)
        counts.append(jnp.where(al == 0, skip + total, 0))
        pick = jnp.zeros_like(sub)
        for j in range(PASSED):
            up = jnp.max(jnp.where(passed[1, dc] == j, slots + ranks[3], 0), axis=0, keepdims=True)
            down = jnp.max(jnp.where(passed[-1, dc] == j, ranks[2], 0), axis=0, keepdims=True)
            up = roll(jnp.broadcast_to(up, sub.shape), grid_c, 1)
            down = roll(jnp.broadcast_to(down, sub.shape), -rows * grid_c, 1)
            pick = jnp.where(sub == j, jnp.maximum(up, down), pick)
        picks.append(pick)
    own = al * slots + sub
    found = []
    for da, dc in STEPS:
        place = own if dc == 0 else jnp.full_like(own, -1)
        for gd in (-1, 0, 1):
            if (da, dc, gd) not in side:
                continue
            if gd and dc:
                base, rank = bases[4 + (dc < 0)], passed[gd, -dc]
            else:
                d = FLOWS.index((gd, -dc))
                base, rank = bases[d], ranks[d]
            there = jnp.where(rank >= 0, rows * slots + base + rank, -1)
            place = jnp.where(side[da, dc, gd], there, place)
        place = sh(place, (da, dc))
        kept = sh(stored, (da, dc))
        loc = jnp.full_like(own, -1)
        for m in range(slots):
            loc = jnp.where(wanted == row_of(kept, m), row_of(place, m), loc)
        found.append(loc)
    locs = []
    for k in range(slots):
        loc = jnp.full_like(own, -1)
        for i in range(len(STEPS)):
            loc = jnp.where(row_of(hits[i], k) > 0, found[i], loc)
        locs.append(loc)
    return locs, ranks, counts, picks


def level_of(counts, levels):
    sizes = []
    for group in (counts[:2], counts[2:4], counts[4:]):
        most = group[0]
        for c in group[1:]:
            most = jnp.maximum(most, c)
        sizes.append(jnp.max(most))
    out = jnp.int32(0)
    for step in levels[:-1]:
        over = sizes[0] > step[0]
        for size, s in zip(sizes[1:], step[1:]):
            over = over | (size > s)
        out = out + over.astype(jnp.int32)
    return out


def my_lanes(rows, grid_c):
    start = lax.axis_index("grp") * rows * grid_c + lax.axis_index("col")
    return [start + i * grid_c for i in range(rows)]


def put_blocks(rank_ref, blocks, send, sem, row, lane, flows, slots, bases, total):
    for d in flows:
        for m in range(slots):
            rank = rank_ref[d * 8 + m, lane]

            @pl.when(rank >= 0)
            def _(d=d, m=m, rank=rank):
                pltpu.make_async_copy(blocks.at[row * slots + m], send.at[bases[d] + rank], sem).start()

            total = total + (rank >= 0).astype(jnp.int32)
    return total


def put_row(rank_ref, blocks, send, sem, row, lanes, rows, slots, bases, total):
    flows = [0, 1]
    if row == 0:
        flows += [2]
    if row == rows - 1:
        flows += [3]
    return put_blocks(rank_ref, blocks, send, sem, row, lanes[row], flows, slots, bases, total)


def drain(n, src, dst, sem):
    def one(_, carry):
        pltpu.make_async_copy(src, dst, sem).wait()
        return carry

    lax.fori_loop(0, n, one, 0)


def plan_kernel(
    dims, cols_ref, filt_ref, x_ref, loc1, loc2, rank2, cnt1, cnt2, pick1, pick2, level, send, rank1_v, rank1, tsem, sem
):
    rows, grid_a, grid_c, slots, levels = dims
    bases, _ = flow_bases(rows, slots)
    cols, filt = cols_ref[...], filt_ref[...]

    def roll(x, s, axis):
        return pltpu.roll(x, s % x.shape[axis], axis)

    maps = grid_maps(cols.shape, grid_a, grid_c, rows)
    hits, uses = chosen(cols, maps, grid_c, roll)
    asked = jnp.where(filt < 0, -2, filt)
    locs, ranks, counts, picks = tables(cols, asked, hits, uses, maps, rows, grid_c, slots, roll)
    for d in range(4):
        rank1_v[d * 8 : d * 8 + 8, :] = ranks[d]
    for d in range(6):
        cnt1[d : d + 1, :] = counts[d][:1]
    for d in range(2):
        pick1[d * 8 : d * 8 + 8, :] = picks[d]
    table = pltpu.make_async_copy(rank1_v, rank1, tsem)
    table.start()
    for k in range(slots):
        loc1[k * 8 : k * 8 + 8, :] = locs[k]
    level[0] = level_of(counts, levels[0])
    table.wait()
    lanes = my_lanes(rows, grid_c)
    total = jnp.int32(0)
    for row in range(rows):
        total = put_row(rank1, x_ref, send, sem, row, lanes, rows, slots, bases, total)
    asked = jnp.where(cols < 0, -2, cols)
    locs, ranks, counts, picks = tables(filt, asked, hits, uses, maps, rows, grid_c, slots, roll)
    for d in range(4):
        rank2[d * 8 : d * 8 + 8, :] = ranks[d]
    for d in range(6):
        cnt2[d : d + 1, :] = counts[d][:1]
    for d in range(2):
        pick2[d * 8 : d * 8 + 8, :] = picks[d]
    for k in range(slots):
        loc2[k * 8 : k * 8 + 8, :] = locs[k]
    level[1] = level_of(counts, levels[1])
    drain(total, x_ref.at[0], send.at[0], sem)


def swap_kernel(sizes, dims, pick, send, recv, edge, passing, send_sem, recv_sem, edge_sem):
    rows, grid_c, slots = dims
    wide, tall, on = sizes
    bases, _ = flow_bases(rows, slots)
    grp, col = lax.axis_index("grp"), lax.axis_index("col")
    grps, cols = lax.axis_size("grp"), lax.axis_size("col")
    barrier = pltpu.get_barrier_semaphore()
    peers = [(lax.rem(grp + gd + grps, grps), lax.rem(col + dc + cols, cols)) for gd, dc in FLOWS]
    for peer in peers:
        pl.semaphore_signal(barrier, inc=1, device_id=peer, device_id_type=MESH)
    pl.semaphore_wait(barrier, 4)

    def start(d, src, dst, peer):
        copy = pltpu.make_async_remote_copy(
            src_ref=src,
            dst_ref=dst,
            send_sem=send_sem.at[d],
            recv_sem=recv_sem.at[d],
            device_id=peer,
            device_id_type=MESH,
        )
        copy.start()
        return copy

    across = [
        start(d, send.at[pl.ds(bases[d], tall)], edge.at[pl.ds((d - 2) * slots, tall)], peers[d]) for d in (2, 3)
    ]
    along = [
        start(d, send.at[pl.ds(bases[d], wide)], recv.at[pl.ds(bases[d], wide)], peers[d]) for d in (0, 1)
    ]
    for copy in across:
        copy.wait()
    lane = grp * rows * grid_c + col
    for d in (0, 1):
        for j in range(on):
            passing[d * PASSED + j] = edge[pick[d * 8 + j, lane]]
    stays = []
    for d in (0, 1):
        stay = pltpu.make_async_copy(
            edge.at[pl.ds(d * slots, tall)], recv.at[pl.ds(bases[2 + d], tall)], edge_sem.at[d]
        )
        stay.start()
        stays.append(stay)
    for d in (0, 1):
        along.append(
            start(4 + d, passing.at[pl.ds(d * PASSED, on)], recv.at[pl.ds(bases[4 + d], on)], peers[d])
        )
    for copy in along + stays:
        copy.wait()


def swap(send, pick, level, levels, rows, grid_c, slots, first_id):
    branches = []
    for sizes in levels:
        branches.append(
            pl.pallas_call(
                functools.partial(swap_kernel, sizes, (rows, grid_c, slots)),
                out_shape=jax.ShapeDtypeStruct(send.shape, send.dtype),
                in_specs=[pl.BlockSpec(memory_space=pltpu.SMEM), pl.BlockSpec(memory_space=pl.ANY)],
                out_specs=pl.BlockSpec(memory_space=pl.ANY),
                scratch_shapes=[
                    pltpu.VMEM((2 * slots,) + send.shape[1:], send.dtype),
                    pltpu.VMEM((2 * PASSED,) + send.shape[1:], send.dtype),
                    pltpu.SemaphoreType.DMA((6,)),
                    pltpu.SemaphoreType.DMA((6,)),
                    pltpu.SemaphoreType.DMA((2,)),
                ],
                compiler_params=pltpu.CompilerParams(
                    collective_id=first_id + len(branches), has_side_effects=True, vmem_limit_bytes=LIMIT
                ),
                name="swap_%d_%d_%d" % sizes,
            )
        )
    return lax.switch(level, branches, pick, send)


def fetch(cnt, recv, buf, sem, rows, grid_c, slots):
    bases, _ = flow_bases(rows, slots)
    grp, col = lax.axis_index("grp"), lax.axis_index("col")
    grps = lax.axis_size("grp")
    total = jnp.int32(0)
    for d, (gd, dc) in enumerate(FLOWS + FLOWS[:2]):
        g = lax.rem(grp - gd + (d >= 4) + grps, grps)
        c = lax.rem(col - dc + grid_c, grid_c)
        n = cnt[d, (g * rows + (rows - 1) * (d < 4)) * grid_c + c]

        def one(i, carry, d=d):
            pltpu.make_async_copy(recv.at[bases[d] + i], buf.at[rows * slots + bases[d] + i], sem).start()
            return carry

        lax.fori_loop(0, n, one, 0)
        total = total + n
    return total


def products(loc, left, buf, acc, row, lane, f, slots):
    acc[...] = jnp.zeros_like(acc)
    for k in range(slots):
        at = loc[k * 8 + f, lane]

        @pl.when(at >= 0)
        def _(k=k, at=at):
            acc[...] += jnp.dot(left[row * slots + k], buf[at], preferred_element_type=jnp.float32)


def square_kernel(dims, loc, cnt, rank2, x, recv, out, send, buf, acc, xsem, sem, ssem):
    rows, grid_c, slots = dims
    bases, _ = flow_bases(rows, slots)
    mine = pltpu.make_async_copy(x, buf.at[pl.ds(0, rows * slots)], xsem)
    mine.start()
    total = fetch(cnt, recv, buf, sem, rows, grid_c, slots)
    mine.wait()
    drain(total, recv.at[0], buf.at[rows * slots], sem)
    lanes = my_lanes(rows, grid_c)
    sent = jnp.int32(0)
    for row in range(rows):

        def one(f, carry, row=row):
            products(loc, buf, buf, acc, row, lanes[row], f, slots)
            out[row * slots + f] = acc[...].astype(out.dtype)
            return carry

        lax.fori_loop(0, slots, one, 0)
        sent = put_row(rank2, out, send, ssem, row, lanes, rows, slots, bases, sent)
    drain(sent, out.at[0], send.at[0], ssem)


def cube_kernel(dims, scale, loc, cnt, cols, x, square, recv, out, buf, acc, xsem, sem):
    rows, grid_c, slots = dims
    mine = pltpu.make_async_copy(square, buf.at[pl.ds(0, rows * slots)], xsem)
    mine.start()
    total = fetch(cnt, recv, buf, sem, rows, grid_c, slots)
    mine.wait()
    drain(total, recv.at[0], buf.at[rows * slots], sem)
    lanes = my_lanes(rows, grid_c)
    for row in range(rows):

        def one(f, carry, row=row):
            products(loc, x, buf, acc, row, lanes[row], f, slots)
            used = (cols[f, lanes[row]] >= 0).astype(jnp.float32)
            value = 1.5 * x[row * slots + f].astype(jnp.float32) - acc[...] * scale
            out[row * slots + f] = (value * used).astype(out.dtype)
            return carry

        lax.fori_loop(0, slots, one, 0)


def local(x_blocks, columns, filter_ids):
    grps, ncol = lax.axis_size("grp"), lax.axis_size("col")
    rows, per_col, slots, order = x_blocks.shape[:4]
    assert per_col == 1 and filter_ids.shape[2] == slots
    grid_a, grid_c = rows * grps, per_col * ncol
    count = grid_a * grid_c
    blocks = x_blocks.reshape(rows * slots, order, order)
    _, extra = flow_bases(rows, slots)
    dtype = blocks.dtype
    most = (rows * slots, slots, PASSED)
    levels = [[tuple(min(n, m) for n, m in zip(sizes, most)) for sizes in steps] + [most] for steps in STAIRS]

    def laid(table):
        return jnp.pad(table.reshape(count, slots).T, ((0, 8 - slots), (0, 0)), constant_values=-1)

    cols, filt = laid(columns), laid(filter_ids)
    vmem = pl.BlockSpec(memory_space=pltpu.VMEM)
    smem = pl.BlockSpec(memory_space=pltpu.SMEM)
    anyw = pl.BlockSpec(memory_space=pl.ANY)
    ints = lambda n: jax.ShapeDtypeStruct((n, count), jnp.int32)
    packed = jax.ShapeDtypeStruct((extra, order, order), dtype)
    held = jax.ShapeDtypeStruct(blocks.shape, dtype)
    dma = pltpu.SemaphoreType.DMA
    params = pltpu.CompilerParams(vmem_limit_bytes=LIMIT)

    loc1, loc2, rank2, cnt1, cnt2, pick1, pick2, level, send = pl.pallas_call(
        functools.partial(plan_kernel, (rows, grid_a, grid_c, slots, levels)),
        out_shape=[
            ints(slots * 8),
            ints(slots * 8),
            ints(32),
            ints(8),
            ints(8),
            ints(16),
            ints(16),
            jax.ShapeDtypeStruct((2,), jnp.int32),
            packed,
        ],
        in_specs=[vmem, vmem, vmem],
        out_specs=[vmem] * 7 + [smem, anyw],
        scratch_shapes=[pltpu.VMEM((32, count), jnp.int32), pltpu.SMEM((32, count), jnp.int32), dma(()), dma(())],
        compiler_params=params,
        name="plan",
    )(cols, filt, blocks)
    recv = swap(send, pick1, level[0], levels[0], rows, grid_c, slots, 0)
    square, send = pl.pallas_call(
        functools.partial(square_kernel, (rows, grid_c, slots)),
        out_shape=[held, packed],
        in_specs=[smem, smem, smem, anyw, anyw],
        out_specs=[vmem, anyw],
        scratch_shapes=[
            pltpu.VMEM((rows * slots + extra, order, order), dtype),
            pltpu.VMEM((order, order), jnp.float32),
            dma(()),
            dma(()),
            dma(()),
        ],
        compiler_params=params,
        name="square",
    )(loc1, cnt1, rank2, blocks, recv)
    recv = swap(send, pick2, level[1], levels[1], rows, grid_c, slots, len(levels[0]))
    out = pl.pallas_call(
        functools.partial(cube_kernel, (rows, grid_c, slots), 0.5 / (slots * order)),
        out_shape=held,
        in_specs=[smem, smem, smem, vmem, anyw, anyw],
        out_specs=vmem,
        scratch_shapes=[
            pltpu.VMEM((rows * slots + extra, order, order), dtype),
            pltpu.VMEM((order, order), jnp.float32),
            dma(()),
            dma(()),
        ],
        compiler_params=params,
        name="cube",
    )(loc2, cnt2, cols, blocks, square, recv)
    return out.reshape(x_blocks.shape)


def solution(mesh):
    return jax.shard_map(
        local,
        mesh=mesh,
        in_specs=(P("grp", "col", None, None, None), P(), P()),
        out_specs=P("grp", "col", None, None, None),
        check_vma=False,
    )
```

```python
import functools

import jax
import jax.numpy as jnp
from jax import lax
from jax.experimental import pallas as pl
from jax.experimental.pallas import tpu as pltpu
from jax.sharding import PartitionSpec as P

MESH = pl.DeviceIdType.MESH
STEPS = [(da, dc) for da in (-1, 0, 1) for dc in (-1, 0, 1)]
FLOWS = [(0, -1), (0, 1), (-1, 0), (1, 0)]
PASSED = 8
BATCH = 4
STAIRS = (
    ((11, 6, 5), (12, 6, 5), (13, 6, 5), (14, 6, 6), (15, 6, 7), (18, 6, 8)),
    ((14, 6, 6), (15, 6, 6), (16, 6, 6), (16, 6, 7), (18, 6, 7), (20, 6, 8)),
)
LIMIT = 48 * 1024 * 1024


def flow_bases(rows, slots):
    sizes = [rows * slots] * 2 + [slots] * 2 + [PASSED] * 2
    bases = [sum(sizes[:i]) for i in range(6)]
    return bases, sum(sizes)


def grid_maps(shape, grid_a, grid_c, rows):
    rid = lax.broadcasted_iota(jnp.int32, shape, 1)
    a = jnp.zeros_like(rid)
    for i in range(1, grid_a):
        a = a + (rid >= i * grid_c).astype(jnp.int32)
    group = jnp.zeros_like(rid)
    for i in range(1, grid_a // rows):
        group = group + (a >= i * rows).astype(jnp.int32)
    return rid, rid - a * grid_c, a - group * rows


def shifted(x, step, col, grid_c, roll):
    da, dc = step
    if da:
        x = roll(x, -da * grid_c, 1)
    if dc == 1:
        x = jnp.where(col == grid_c - 1, roll(x, grid_c - 1, 1), roll(x, -1, 1))
    if dc == -1:
        x = jnp.where(col == 0, roll(x, 1 - grid_c, 1), roll(x, 1, 1))
    return x


def row_of(x, i):
    return jnp.broadcast_to(x[i : i + 1], x.shape)


def chosen(cols, maps, grid_c, roll):
    rid, col, _ = maps
    hits, uses = [], []
    for step in STEPS:
        hit = (cols == shifted(rid, step, col, grid_c, roll)).astype(jnp.int32)
        hits.append(hit)
        uses.append(jnp.broadcast_to(jnp.max(hit, axis=0, keepdims=True), cols.shape))
    return hits, uses


def tables(stored, wanted, hits, uses, maps, rows, grid_c, slots, roll):
    _, col, al = maps
    sub = lax.broadcasted_iota(jnp.int32, stored.shape, 0)
    bases, _ = flow_bases(rows, slots)
    sh = functools.partial(shifted, col=col, grid_c=grid_c, roll=roll)
    need = {(gd, dc): jnp.zeros_like(stored) for gd in (-1, 0, 1) for dc in (-1, 0, 1)}
    side = {}
    for i, (da, dc) in enumerate(STEPS):
        back = (-da, -dc)
        asked = sh(wanted, back)
        hit = jnp.zeros_like(stored)
        for f in range(slots):
            hit = hit | (stored == row_of(asked, f)).astype(jnp.int32)
        hit = hit & sh(uses[i], back)
        for gd in (-1, 0, 1):
            if (gd, -dc) == (0, 0) or gd * da > 0 or (gd != 0 and da == 0):
                continue
            at = al - da
            inside = (at < 0) if gd < 0 else (at >= rows) if gd > 0 else (at >= 0) & (at < rows)
            side[da, dc, gd] = inside
            need[gd, -dc] = need[gd, -dc] | (hit & inside.astype(jnp.int32))
    def ahead_of(n):
        ahead = jnp.zeros_like(n)
        for s in range(1, slots):
            ahead = ahead + jnp.where(sub >= s, roll(n, s, 0), 0)
        return ahead, jnp.broadcast_to(jnp.sum(n, axis=0, keepdims=True), n.shape)

    ranks, counts = [], []
    for gd, dc in FLOWS:
        n = need[gd, dc]
        if gd:
            n = n | need[gd, -1] | need[gd, 1]
        ahead, total = ahead_of(n)
        before = jnp.zeros_like(n)
        for s in range(1, rows):
            before = before + jnp.where(al >= s, roll(total, s * grid_c, 1), 0)
        ranks.append(jnp.where(n > 0, before + ahead, -1))
        counts.append(jnp.where(al == rows - 1, before + total, 0))
    passed, picks = {}, []
    for dc in (-1, 1):
        low, high = need[1, dc], need[-1, dc]
        ahead, total = ahead_of(low)
        passed[1, dc] = jnp.where(low > 0, ahead, -1)
        skip = roll(total, (rows + 1) * grid_c, 1)
        ahead, total = ahead_of(high)
        passed[-1, dc] = jnp.where(high > 0, ahead + skip, -1)
        counts.append(jnp.where(al == 0, skip + total, 0))
        pick = jnp.zeros_like(sub)
        for j in range(PASSED):
            up = jnp.max(jnp.where(passed[1, dc] == j, slots + ranks[3], 0), axis=0, keepdims=True)
            down = jnp.max(jnp.where(passed[-1, dc] == j, ranks[2], 0), axis=0, keepdims=True)
            up = roll(jnp.broadcast_to(up, sub.shape), grid_c, 1)
            down = roll(jnp.broadcast_to(down, sub.shape), -rows * grid_c, 1)
            pick = jnp.where(sub == j, jnp.maximum(up, down), pick)
        picks.append(pick)
    own = al * slots + sub
    found = []
    for da, dc in STEPS:
        place = own if dc == 0 else jnp.full_like(own, -1)
        for gd in (-1, 0, 1):
            if (da, dc, gd) not in side:
                continue
            if gd and dc:
                base, rank = bases[4 + (dc < 0)], passed[gd, -dc]
            else:
                d = FLOWS.index((gd, -dc))
                base, rank = bases[d], ranks[d]
            there = jnp.where(rank >= 0, rows * slots + base + rank, -1)
            place = jnp.where(side[da, dc, gd], there, place)
        place = sh(place, (da, dc))
        kept = sh(stored, (da, dc))
        loc = jnp.full_like(own, -1)
        for m in range(slots):
            loc = jnp.where(wanted == row_of(kept, m), row_of(place, m), loc)
        found.append(loc)
    locs = []
    for k in range(slots):
        loc = jnp.full_like(own, -1)
        for i in range(len(STEPS)):
            loc = jnp.where(row_of(hits[i], k) > 0, found[i], loc)
        locs.append(loc)
    return locs, ranks, counts, picks


def level_of(counts, levels):
    sizes = []
    for group in (counts[:2], counts[2:4], counts[4:]):
        most = group[0]
        for c in group[1:]:
            most = jnp.maximum(most, c)
        sizes.append(jnp.max(most))
    out = jnp.int32(0)
    for step in levels[:-1]:
        over = sizes[0] > step[0]
        for size, s in zip(sizes[1:], step[1:]):
            over = over | (size > s)
        out = out + over.astype(jnp.int32)
    return out


def my_lanes(rows, grid_c):
    start = lax.axis_index("grp") * rows * grid_c + lax.axis_index("col")
    return [start + i * grid_c for i in range(rows)]


def put_blocks(rank_ref, blocks, send, sem, row, lane, flows, slots, bases, total):
    for d in flows:
        for m in range(slots):
            rank = rank_ref[d * 8 + m, lane]

            @pl.when(rank >= 0)
            def _(d=d, m=m, rank=rank):
                pltpu.make_async_copy(blocks.at[row * slots + m], send.at[bases[d] + rank], sem).start()

            total = total + (rank >= 0).astype(jnp.int32)
    return total


def put_row(rank_ref, blocks, send, sem, row, lanes, rows, slots, bases, total):
    flows = [0, 1]
    if row == 0:
        flows += [2]
    if row == rows - 1:
        flows += [3]
    return put_blocks(rank_ref, blocks, send, sem, row, lanes[row], flows, slots, bases, total)


def drain(n, src, dst, sem):
    def one(_, carry):
        pltpu.make_async_copy(src, dst, sem).wait()
        return carry

    lax.fori_loop(0, n, one, 0)


def plan_kernel(
    dims, cols_ref, filt_ref, x_ref, loc1, loc2, rank2, cnt1, cnt2, pick1, pick2, level, send, rank1_v, rank1, tsem, sem
):
    rows, grid_a, grid_c, slots, levels = dims
    bases, _ = flow_bases(rows, slots)
    cols, filt = cols_ref[...], filt_ref[...]

    def roll(x, s, axis):
        return pltpu.roll(x, s % x.shape[axis], axis)

    maps = grid_maps(cols.shape, grid_a, grid_c, rows)
    hits, uses = chosen(cols, maps, grid_c, roll)
    asked = jnp.where(filt < 0, -2, filt)
    locs, ranks, counts, picks = tables(cols, asked, hits, uses, maps, rows, grid_c, slots, roll)
    for d in range(4):
        rank1_v[d * 8 : d * 8 + 8, :] = ranks[d]
    for d in range(6):
        cnt1[d : d + 1, :] = counts[d][:1]
    for d in range(2):
        pick1[d * 8 : d * 8 + 8, :] = picks[d]
    table = pltpu.make_async_copy(rank1_v, rank1, tsem)
    table.start()
    for k in range(slots):
        loc1[k * 8 : k * 8 + 8, :] = locs[k]
    level[0] = level_of(counts, levels[0])
    table.wait()
    lanes = my_lanes(rows, grid_c)
    total = jnp.int32(0)
    for row in range(rows):
        total = put_row(rank1, x_ref, send, sem, row, lanes, rows, slots, bases, total)
    asked = jnp.where(cols < 0, -2, cols)
    locs, ranks, counts, picks = tables(filt, asked, hits, uses, maps, rows, grid_c, slots, roll)
    for d in range(4):
        rank2[d * 8 : d * 8 + 8, :] = ranks[d]
    for d in range(6):
        cnt2[d : d + 1, :] = counts[d][:1]
    for d in range(2):
        pick2[d * 8 : d * 8 + 8, :] = picks[d]
    for k in range(slots):
        loc2[k * 8 : k * 8 + 8, :] = locs[k]
    level[1] = level_of(counts, levels[1])
    drain(total, x_ref.at[0], send.at[0], sem)


def swap_kernel(sizes, dims, pick, send, recv, edge, passing, send_sem, recv_sem, edge_sem):
    rows, grid_c, slots = dims
    wide, tall, on = sizes
    bases, _ = flow_bases(rows, slots)
    grp, col = lax.axis_index("grp"), lax.axis_index("col")
    grps, cols = lax.axis_size("grp"), lax.axis_size("col")
    barrier = pltpu.get_barrier_semaphore()
    peers = [(lax.rem(grp + gd + grps, grps), lax.rem(col + dc + cols, cols)) for gd, dc in FLOWS]
    for peer in peers:
        pl.semaphore_signal(barrier, inc=1, device_id=peer, device_id_type=MESH)
    pl.semaphore_wait(barrier, 4)

    def start(d, src, dst, peer):
        copy = pltpu.make_async_remote_copy(
            src_ref=src,
            dst_ref=dst,
            send_sem=send_sem.at[d],
            recv_sem=recv_sem.at[d],
            device_id=peer,
            device_id_type=MESH,
        )
        copy.start()
        return copy

    across = [
        start(d, send.at[pl.ds(bases[d], tall)], edge.at[pl.ds((d - 2) * slots, tall)], peers[d]) for d in (2, 3)
    ]
    along = [
        start(d, send.at[pl.ds(bases[d], wide)], recv.at[pl.ds(bases[d], wide)], peers[d]) for d in (0, 1)
    ]
    for copy in across:
        copy.wait()
    lane = grp * rows * grid_c + col
    for d in (0, 1):
        for j in range(on):
            passing[d * PASSED + j] = edge[pick[d * 8 + j, lane]]
    stays = []
    for d in (0, 1):
        stay = pltpu.make_async_copy(
            edge.at[pl.ds(d * slots, tall)], recv.at[pl.ds(bases[2 + d], tall)], edge_sem.at[d]
        )
        stay.start()
        stays.append(stay)
    for d in (0, 1):
        along.append(
            start(4 + d, passing.at[pl.ds(d * PASSED, on)], recv.at[pl.ds(bases[4 + d], on)], peers[d])
        )
    for copy in along + stays:
        copy.wait()


def swap(send, pick, level, levels, rows, grid_c, slots, first_id):
    branches = []
    for sizes in levels:
        branches.append(
            pl.pallas_call(
                functools.partial(swap_kernel, sizes, (rows, grid_c, slots)),
                out_shape=jax.ShapeDtypeStruct(send.shape, send.dtype),
                in_specs=[pl.BlockSpec(memory_space=pltpu.SMEM), pl.BlockSpec(memory_space=pl.ANY)],
                out_specs=pl.BlockSpec(memory_space=pl.ANY),
                scratch_shapes=[
                    pltpu.VMEM((2 * slots,) + send.shape[1:], send.dtype),
                    pltpu.VMEM((2 * PASSED,) + send.shape[1:], send.dtype),
                    pltpu.SemaphoreType.DMA((6,)),
                    pltpu.SemaphoreType.DMA((6,)),
                    pltpu.SemaphoreType.DMA((2,)),
                ],
                compiler_params=pltpu.CompilerParams(
                    collective_id=first_id + len(branches), has_side_effects=True, vmem_limit_bytes=LIMIT
                ),
                name="swap_%d_%d_%d" % sizes,
            )
        )
    return lax.switch(level, branches, pick, send)


def fetch(cnt, recv, buf, sem, rows, grid_c, slots):
    bases, _ = flow_bases(rows, slots)
    grp, col = lax.axis_index("grp"), lax.axis_index("col")
    grps = lax.axis_size("grp")
    total = jnp.int32(0)
    for d, (gd, dc) in enumerate(FLOWS + FLOWS[:2]):
        g = lax.rem(grp - gd + (d >= 4) + grps, grps)
        c = lax.rem(col - dc + grid_c, grid_c)
        n = cnt[d, (g * rows + (rows - 1) * (d < 4)) * grid_c + c]

        def one(i, carry, d=d):
            pltpu.make_async_copy(recv.at[bases[d] + i], buf.at[rows * slots + bases[d] + i], sem).start()
            return carry

        lax.fori_loop(0, n, one, 0)
        total = total + n
    return total


def list_jobs(loc, jobs, acc, rows, lanes, slots):
    def clear(i, carry):
        acc[i] = jnp.zeros_like(acc[i])
        return carry

    lax.fori_loop(0, acc.shape[0], clear, 0)
    n = jnp.int32(0)
    for row in range(rows):

        def one(f, n, row=row):
            for k in range(slots):
                at = loc[k * 8 + f, lanes[row]]
                jobs[0, n] = row * slots + k
                jobs[1, n] = at
                jobs[2, n] = row * slots + f
                n = n + (at >= 0).astype(jnp.int32)
            return n

        n = lax.fori_loop(0, slots, one, n)
    for i in range(BATCH):
        jobs[0, n + i] = 0
        jobs[1, n + i] = 0
        jobs[2, n + i] = rows * slots
    return n


def multiply(jobs, n, left, buf, acc):
    def one(i, carry):
        at = i * BATCH
        terms = [
            jnp.dot(left[jobs[0, at + j]], buf[jobs[1, at + j]], preferred_element_type=jnp.float32)
            for j in range(BATCH)
        ]
        for j in range(BATCH):
            acc[jobs[2, at + j]] += terms[j]
        return carry

    lax.fori_loop(0, lax.div(n + BATCH - 1, BATCH), one, 0)


def square_kernel(dims, loc, cnt, rank2, x, recv, out, send, buf, acc, jobs, xsem, sem, ssem):
    rows, grid_c, slots = dims
    bases, _ = flow_bases(rows, slots)
    mine = pltpu.make_async_copy(x, buf.at[pl.ds(0, rows * slots)], xsem)
    mine.start()
    total = fetch(cnt, recv, buf, sem, rows, grid_c, slots)
    lanes = my_lanes(rows, grid_c)
    n = list_jobs(loc, jobs, acc, rows, lanes, slots)
    mine.wait()
    drain(total, recv.at[0], buf.at[rows * slots], sem)
    multiply(jobs, n, buf, buf, acc)
    sent = jnp.int32(0)
    for row in range(rows):

        def one(f, carry, row=row):
            out[row * slots + f] = acc[row * slots + f].astype(out.dtype)
            return carry

        lax.fori_loop(0, slots, one, 0)
        sent = put_row(rank2, out, send, ssem, row, lanes, rows, slots, bases, sent)
    drain(sent, out.at[0], send.at[0], ssem)


def cube_kernel(dims, scale, loc, cnt, cols, x, square, recv, out, buf, acc, jobs, xsem, sem):
    rows, grid_c, slots = dims
    mine = pltpu.make_async_copy(square, buf.at[pl.ds(0, rows * slots)], xsem)
    mine.start()
    total = fetch(cnt, recv, buf, sem, rows, grid_c, slots)
    lanes = my_lanes(rows, grid_c)
    n = list_jobs(loc, jobs, acc, rows, lanes, slots)
    mine.wait()
    drain(total, recv.at[0], buf.at[rows * slots], sem)
    multiply(jobs, n, x, buf, acc)
    for row in range(rows):

        def one(f, carry, row=row):
            used = (cols[f, lanes[row]] >= 0).astype(jnp.float32)
            value = 1.5 * x[row * slots + f].astype(jnp.float32) - acc[row * slots + f] * scale
            out[row * slots + f] = (value * used).astype(out.dtype)
            return carry

        lax.fori_loop(0, slots, one, 0)


def local(x_blocks, columns, filter_ids):
    grps, ncol = lax.axis_size("grp"), lax.axis_size("col")
    rows, per_col, slots, order = x_blocks.shape[:4]
    assert per_col == 1 and filter_ids.shape[2] == slots
    grid_a, grid_c = rows * grps, per_col * ncol
    count = grid_a * grid_c
    blocks = x_blocks.reshape(rows * slots, order, order)
    _, extra = flow_bases(rows, slots)
    dtype = blocks.dtype
    most = (rows * slots, slots, PASSED)
    levels = [[tuple(min(n, m) for n, m in zip(sizes, most)) for sizes in steps] + [most] for steps in STAIRS]

    def laid(table):
        return jnp.pad(table.reshape(count, slots).T, ((0, 8 - slots), (0, 0)), constant_values=-1)

    cols, filt = laid(columns), laid(filter_ids)
    vmem = pl.BlockSpec(memory_space=pltpu.VMEM)
    smem = pl.BlockSpec(memory_space=pltpu.SMEM)
    anyw = pl.BlockSpec(memory_space=pl.ANY)
    ints = lambda n: jax.ShapeDtypeStruct((n, count), jnp.int32)
    packed = jax.ShapeDtypeStruct((extra, order, order), dtype)
    held = jax.ShapeDtypeStruct(blocks.shape, dtype)
    dma = pltpu.SemaphoreType.DMA
    params = pltpu.CompilerParams(vmem_limit_bytes=LIMIT)

    loc1, loc2, rank2, cnt1, cnt2, pick1, pick2, level, send = pl.pallas_call(
        functools.partial(plan_kernel, (rows, grid_a, grid_c, slots, levels)),
        out_shape=[
            ints(slots * 8),
            ints(slots * 8),
            ints(32),
            ints(8),
            ints(8),
            ints(16),
            ints(16),
            jax.ShapeDtypeStruct((2,), jnp.int32),
            packed,
        ],
        in_specs=[vmem, vmem, vmem],
        out_specs=[vmem] * 7 + [smem, anyw],
        scratch_shapes=[pltpu.VMEM((32, count), jnp.int32), pltpu.SMEM((32, count), jnp.int32), dma(()), dma(())],
        compiler_params=params,
        name="plan",
    )(cols, filt, blocks)
    recv = swap(send, pick1, level[0], levels[0], rows, grid_c, slots, 0)
    square, send = pl.pallas_call(
        functools.partial(square_kernel, (rows, grid_c, slots)),
        out_shape=[held, packed],
        in_specs=[smem, smem, smem, anyw, anyw],
        out_specs=[vmem, anyw],
        scratch_shapes=[
            pltpu.VMEM((rows * slots + extra, order, order), dtype),
            pltpu.VMEM((rows * slots + 1, order, order), jnp.float32),
            pltpu.SMEM((3, rows * slots * slots + BATCH), jnp.int32),
            dma(()),
            dma(()),
            dma(()),
        ],
        compiler_params=params,
        name="square",
    )(loc1, cnt1, rank2, blocks, recv)
    recv = swap(send, pick2, level[1], levels[1], rows, grid_c, slots, len(levels[0]))
    out = pl.pallas_call(
        functools.partial(cube_kernel, (rows, grid_c, slots), 0.5 / (slots * order)),
        out_shape=held,
        in_specs=[smem, smem, smem, vmem, anyw, anyw],
        out_specs=vmem,
        scratch_shapes=[
            pltpu.VMEM((rows * slots + extra, order, order), dtype),
            pltpu.VMEM((rows * slots + 1, order, order), jnp.float32),
            pltpu.SMEM((3, rows * slots * slots + BATCH), jnp.int32),
            dma(()),
            dma(()),
        ],
        compiler_params=params,
        name="cube",
    )(loc2, cnt2, cols, blocks, square, recv)
    return out.reshape(x_blocks.shape)


def solution(mesh):
    return jax.shard_map(
        local,
        mesh=mesh,
        in_specs=(P("grp", "col", None, None, None), P(), P()),
        out_specs=P("grp", "col", None, None, None),
        check_vma=False,
    )
```
